32 devices in a mesh: lat: 8 (over z, x), depth: 4 (over y, core).
Axes of the slice: x: 2, y: 2, z: 4, core: 2. Of those that a mesh axis runs over, the one named last changes fastest.
Arguments:
- surface: float32 [128, 4096], P('lat'), may hold values from -6 to 6
- velocity: float32 [2, 128, 4096], P(None, 'lat'), may hold values from -6 to 6
- block_map: int32 [128, 4096], P('lat'), may hold values from 0 to 15
- free_flags: int32 [128, 4096], P('lat'), may hold values 0 or 1
- block_rates: float32 [16], replicated, may hold values from 0.2 to 2
- previous_mesh: float32 [128, 64, 4096], P('lat', 'depth'), may hold values from -6 to 6
Outputs:
- new_surface: float32 [128, 4096], P('lat')
- mesh_field: float32 [128, 64, 4096], P('lat', 'depth')
- column_norm: float32 [128], P('lat')
The draws below stay inside these ranges and needn't reach their ends.
All inputs are finite; a program needn't handle non-finite values. No bound on the sum of `free_flags` on one device may be relied on, other than what follows from the above.
Results may differ from the reference program's by a relative error of at most 0.00002.
Values sent between devices are 32-bit elements; how exact they have to be, the bound alone decides.
A program may use at most 64 MiB of HBM per device.

```python
import math
import jax
import jax.numpy as jnp
from jax import lax

NY = 4096
NB = 16
ITERS = 2
NX = 128
NZ = 64


def touch_ends(result, key, least, top_value):
    place = [jax.random.randint(jax.random.fold_in(key, axis), (), 0, length) for axis, length in enumerate(result.shape)]
    main_axis = result.shape.index(max(result.shape))
    next_to = place[:main_axis] + [(place[main_axis] + 1) % result.shape[main_axis]] + place[main_axis + 1:]
    return result.at[tuple(place)].set(least).at[tuple(next_to)].set(top_value)


def shard_levels(stream_key, extent, cuts, low, largest):
    loudness = 1.0
    for position, parts in cuts:
        heights = jax.random.uniform(jax.random.fold_in(jax.random.fold_in(stream_key, 6), position), (parts,), jnp.float32, low / len(cuts), largest / len(cuts))
        loudness = loudness * jnp.repeat(jnp.exp(heights), extent[position] // parts).reshape((-1,) + (1,) * (len(extent) - 1 - position))
    return loudness


def bell_draw(key, extent, width, most, split=(), held_as=jnp.bfloat16):
    level = shard_levels(key, extent, split, -0.22, 0.18) if split else 1.0
    result = jax.random.normal(key, extent, jnp.float32) * width * level
    return jnp.minimum(jnp.maximum(result, -most), most).astype(held_as)


def setup_inputs(seed: int = 0) -> dict:
    keys = jax.random.split(jax.random.key(seed), 7)
    return {
        "surface": bell_draw(keys[0], (NX, NY), 1.0, 6.0, ((0, 8),), jnp.float32),
        "velocity": bell_draw(keys[1], (2, NX, NY), 1.0, 6.0, ((1, 8),), jnp.float32),
        "block_map": touch_ends(jax.random.randint(keys[2], (NX, NY), 0, NB), jax.random.fold_in(keys[2], 1), 0, NB - 1).astype(jnp.int32),
        "free_flags": touch_ends((jax.random.randint(keys[3], (NX, NY), 0, 4) < 3).astype(jnp.int32), jax.random.fold_in(keys[3], 1), 0, 1),
        "block_rates": jnp.clip(jnp.exp(jax.random.uniform(keys[4], (NB,), jnp.float32, math.log(0.2), math.log(2.0))), 0.2, 2.0),
        "previous_mesh": bell_draw(keys[5], (NX, NZ, NY), 1.0, 6.0, ((0, 8), (1, 4)), jnp.float32),
    }


TIME_STEP = 0.5
RELAX_WEIGHT = 0.8

def relax_once(field, surface_shift):
    padded_rows = jnp.pad(field, ((1, 1), (0, 0), (0, 0)))
    across_rows = padded_rows[2:] + padded_rows[:-2]
    padded_cols = jnp.pad(field, ((0, 0), (0, 0), (1, 1)))
    across_cols = padded_cols[:, :, 2:] + padded_cols[:, :, :-2]
    upper = jnp.concatenate([surface_shift[:, None, :], field[:, :-1, :]], axis=1)
    lower = jnp.concatenate([field[:, 1:, :], jnp.zeros_like(field[:, :1, :])], axis=1)
    neighbours = across_rows + across_cols + upper + lower
    return (1.0 - RELAX_WEIGHT) * field + RELAX_WEIGHT * neighbours / 6.0

def reference(surface, velocity, block_map, free_flags, block_rates, previous_mesh):
    padded = jnp.pad(surface, 1)
    grad_rows = (padded[2:, 1:-1] - padded[:-2, 1:-1]) * 0.5
    grad_cols = (padded[1:-1, 2:] - padded[1:-1, :-2]) * 0.5
    laplace = padded[2:, 1:-1] + padded[:-2, 1:-1] + padded[1:-1, 2:] + padded[1:-1, :-2] - 4.0 * surface
    diffusivity = block_rates[block_map]
    tendency = -velocity[0] * grad_rows - velocity[1] * grad_cols + diffusivity * laplace
    new_surface = surface + TIME_STEP * free_flags.astype(jnp.float32) * tendency
    surface_shift = new_surface - surface
    layers = jnp.arange(NZ, dtype=jnp.int32)
    profile = (NZ - layers).astype(jnp.float32) / NZ
    field = previous_mesh + surface_shift[:, None, :] * profile[None, :, None]
    for sweep_index in range(ITERS):
        field = relax_once(field, surface_shift)
    column_norm = jnp.sqrt(lax.optimization_barrier(jnp.sum(field * field, axis=(1, 2))) / (NZ * NY))
    return (new_surface, field, column_norm)
```

```python
import functools

import jax
import jax.numpy as jnp
from jax import lax
from jax.experimental import pallas as pl
from jax.experimental.pallas import tpu as pltpu
from jax.sharding import PartitionSpec as P

ITERS = 2
TIME_STEP = 0.5
RELAX_WEIGHT = 0.8
MESH = pl.DeviceIdType.MESH
PAD = 128
TILE = 8
WIDTH = 512
CHUNKS = 4
EARLY = 3
SURF, SHIFT, FIRST = 0, 1, 2


def lanes_beside(window, width):
    span = window.shape[1]
    left = pltpu.roll(window, 1, 1)[:, PAD : PAD + width]
    right = pltpu.roll(window, span - 1, 1)[:, PAD : PAD + width]
    return window[:, PAD : PAD + width], left, right


def kernel(
    lats,
    depths,
    surface,
    velocity,
    block_map,
    free_flags,
    rates,
    previous,
    new_surface,
    field,
    norm,
    surf,
    vel,
    blocks,
    flags,
    shift,
    moved,
    first,
    second,
    result,
    squares,
    sums,
    others,
    local_sem,
    out_sem,
    lat_send,
    lat_recv,
    depth_send,
    depth_recv,
    sum_send,
    sum_recv,
):
    rows, layers, columns = previous.shape
    lat = lax.axis_index("lat")
    depth = lax.axis_index("depth")
    total_layers = layers * depths
    blocks_count = rates.shape[0]
    steps = columns // WIDTH
    piece = columns // CHUNKS
    has_low, has_high = lat > 0, lat < lats - 1
    has_above, has_below = depth > 0, depth < depths - 1
    body_rows = pl.ds(TILE, rows)
    body_layers = pl.ds(TILE, layers)
    body_cols = pl.ds(PAD, columns)

    locals_ = [
        pltpu.make_async_copy(surface, surf.at[body_rows, body_cols], local_sem.at[0]),
        pltpu.make_async_copy(velocity, vel, local_sem.at[1]),
        pltpu.make_async_copy(block_map, blocks, local_sem.at[2]),
        pltpu.make_async_copy(free_flags, flags, local_sem.at[3]),
        pltpu.make_async_copy(
            previous, first.at[pl.ds(1, rows), body_layers, body_cols], local_sem.at[4]
        ),
    ]
    for copy in locals_:
        copy.start()

    barrier = pltpu.get_barrier_semaphore()

    def greet(target):
        pl.semaphore_signal(barrier, inc=1, device_id=target, device_id_type=MESH)

    low_id = {"lat": jnp.maximum(lat - 1, 0)}
    high_id = {"lat": jnp.minimum(lat + 1, lats - 1)}
    above_id = {"depth": jnp.maximum(depth - 1, 0)}
    below_id = {"depth": jnp.minimum(depth + 1, depths - 1)}

    pl.when(has_low)(lambda: greet(low_id))
    pl.when(has_high)(lambda: greet(high_id))
    for k in range(1, depths):
        greet({"depth": lax.rem(depth + k, depths)})
    peers = depths - 1 + has_low.astype(jnp.int32) + has_high.astype(jnp.int32)
    pl.semaphore_wait(barrier, peers)

    def lateral(side, slot, src, dst):
        return pltpu.make_async_remote_copy(
            src_ref=src,
            dst_ref=dst,
            send_sem=lat_send.at[side, slot],
            recv_sem=lat_recv.at[side, slot],
            device_id=high_id if side == 0 else low_id,
            device_id_type=MESH,
        )

    def vertical(side, slot, src, dst):
        return pltpu.make_async_remote_copy(
            src_ref=src,
            dst_ref=dst,
            send_sem=depth_send.at[side, slot],
            recv_sem=depth_recv.at[side, slot],
            device_id=below_id if side == 0 else above_id,
            device_id_type=MESH,
        )

    def piece_cols(k):
        return pl.ds(PAD + k * piece, piece)

    lat_sends = (has_high, has_low)
    lat_recvs = (has_low, has_high)
    depth_sends = (has_below, has_above)
    depth_recvs = (has_above, has_below)
    own_edge = (rows, 1)
    far_edge = (0, rows + 1)
    own_layer = (TILE + layers - 1, TILE)
    far_layer = (TILE - 1, TILE + layers)

    surf_copies = [
        lateral(
            side,
            SURF,
            surface.at[pl.ds((rows - 1, 0)[side], 1), :],
            surf.at[pl.ds((TILE - 1, TILE + rows)[side], 1), body_cols],
        )
        for side in (0, 1)
    ]
    shift_copies = [
        lateral(
            side,
            SHIFT,
            shift.at[pl.ds((TILE + rows - 1, TILE)[side], 1), :],
            shift.at[pl.ds((TILE - 1, TILE + rows)[side], 1), :],
        )
        for side in (0, 1)
    ]
    first_copies = [
        [
            lateral(
                side,
                FIRST + k,
                previous.at[(rows - 1, 0)[side], :, pl.ds(k * piece, piece)],
                first.at[far_edge[side], body_layers, piece_cols(k)],
            )
            for side in (0, 1)
        ]
        for k in range(CHUNKS)
    ]
    second_copies = [
        [
            lateral(
                side,
                FIRST + CHUNKS + k,
                second.at[own_edge[side], body_layers, piece_cols(k)],
                second.at[far_edge[side], body_layers, piece_cols(k)],
            )
            for side in (0, 1)
        ]
        for k in range(CHUNKS)
    ]
    layer_copies = [
        vertical(
            side,
            0,
            previous.at[:, pl.ds((layers - 1, 0)[side], 1), :],
            first.at[pl.ds(1, rows), pl.ds(far_layer[side], 1), body_cols],
        )
        for side in (0, 1)
    ]
    spans = (pl.ds(2, rows - 2), pl.ds(1, 1), pl.ds(rows, 1))
    later_layers = [
        [
            vertical(
                side,
                1 + j,
                second.at[span, pl.ds(own_layer[side], 1), body_cols],
                second.at[span, pl.ds(far_layer[side], 1), body_cols],
            )
            for side in (0, 1)
        ]
        for j, span in enumerate(spans)
    ]
    sum_copies = [
        pltpu.make_async_remote_copy(
            src_ref=sums,
            dst_ref=others.at[k - 1],
            send_sem=sum_send.at[k - 1],
            recv_sem=sum_recv.at[k - 1],
            device_id={"depth": lax.rem(depth + k, depths)},
            device_id_type=MESH,
        )
        for k in range(1, depths)
    ]

    for side in (0, 1):
        pl.when(lat_sends[side])(surf_copies[side].start)
    for side in (0, 1):
        pl.when(depth_sends[side])(layer_copies[side].start)
    for k in range(EARLY):
        for side in (0, 1):
            pl.when(lat_sends[side])(first_copies[k][side].start)

    zero_tile = jnp.zeros((layers, PAD), jnp.float32)

    def clear_pads(r, carry):
        for buffer in (first, second):
            for start in (0, PAD + columns):
                buffer[r, body_layers, pl.ds(start, PAD)] = zero_tile
        return carry

    lax.fori_loop(1, rows + 1, clear_pads, 0)
    for start in (0, PAD + columns):
        surf[body_rows, pl.ds(start, PAD)] = jnp.zeros((rows, PAD), jnp.float32)
    squares[...] = jnp.zeros_like(squares)

    for side in (0, 1):

        @pl.when(jnp.logical_not(lat_recvs[side]))
        def _(side=side):
            surf[pl.ds((TILE - 1, TILE + rows)[side], 1), body_cols] = jnp.zeros(
                (1, columns), jnp.float32
            )
            shift[pl.ds((TILE - 1, TILE + rows)[side], 1), :] = jnp.zeros(
                (1, columns), jnp.float32
            )
            for buffer in (first, second):
                buffer[far_edge[side], body_layers, body_cols] = jnp.zeros(
                    (layers, columns), jnp.float32
                )

    for copy in locals_[:4]:
        copy.wait()
    for side in (0, 1):
        pl.when(lat_recvs[side])(surf_copies[side].wait_recv)

    def advect(step, carry):
        c = pl.multiple_of(step * WIDTH, WIDTH)
        cols = pl.ds(c, WIDTH)
        inner = pl.ds(pl.multiple_of(c + PAD, PAD), WIDTH)
        middle, left, right = lanes_beside(surf[body_rows, pl.ds(c, WIDTH + 2 * PAD)], WIDTH)
        before = pltpu.roll(surf[pl.ds(0, rows + TILE), inner], 1, 0)[TILE:]
        after = pltpu.roll(surf[pl.ds(TILE, rows + TILE), inner], rows + TILE - 1, 0)[:rows]
        grad_rows = (after - before) * 0.5
        grad_cols = (right - left) * 0.5
        laplace = after + before + right + left - 4.0 * middle
        names = blocks[:, cols]
        rate = jnp.full(names.shape, rates[0], jnp.float32)
        for label in range(1, blocks_count):
            rate = jnp.where(names == label, rates[label], rate)
        tendency = -vel[0, :, cols] * grad_rows - vel[1, :, cols] * grad_cols + rate * laplace
        fresh = middle + TIME_STEP * flags[:, cols].astype(jnp.float32) * tendency
        moved[:, cols] = fresh
        shift[body_rows, cols] = fresh - middle
        return carry

    lax.fori_loop(0, steps, advect, 0)
    surface_out = pltpu.make_async_copy(moved, new_surface, out_sem.at[0])
    surface_out.start()
    locals_[4].wait()
    for side in (0, 1):
        pl.when(lat_sends[side])(shift_copies[side].start)
    for k in range(EARLY, CHUNKS):
        for side in (0, 1):
            pl.when(lat_sends[side])(first_copies[k][side].start)

    for side in (0, 1):
        pl.when(depth_recvs[side])(layer_copies[side].wait_recv)

    def profile_of(index):
        return (total_layers - index).astype(jnp.float32) / total_layers

    base = depth * layers
    profile = profile_of(base + lax.broadcasted_iota(jnp.int32, (layers, WIDTH), 0))
    above_profile = profile_of(base - 1)
    below_profile = profile_of(base + layers)

    def widen(r, c, top, bottom):
        cols = pl.ds(c, WIDTH)
        inner = pl.ds(pl.multiple_of(c + PAD, PAD), WIDTH)
        row_shift = shift[pl.ds(TILE - 1 + r, 1), cols]
        first[r, body_layers, inner] = (
            first[r, body_layers, inner] + jnp.broadcast_to(row_shift, (layers, WIDTH)) * profile
        )
        if top is not None:
            top(r, inner, row_shift)
            bottom(r, inner, row_shift)

    above = pl.ds(TILE - 1, 1)
    below = pl.ds(TILE + layers, 1)

    def own_rows(t, carry):
        r = t // steps + 1
        c = pl.multiple_of(lax.rem(t, steps) * WIDTH, WIDTH)

        def top(r, inner, row_shift):
            @pl.when(has_above)
            def _():
                first[r, above, inner] = first[r, above, inner] + row_shift * above_profile

            @pl.when(jnp.logical_not(has_above))
            def _():
                first[r, above, inner] = row_shift
                second[r, above, inner] = row_shift

        def bottom(r, inner, row_shift):
            @pl.when(has_below)
            def _():
                first[r, below, inner] = first[r, below, inner] + row_shift * below_profile

            @pl.when(jnp.logical_not(has_below))
            def _():
                first[r, below, inner] = jnp.zeros_like(row_shift)
                second[r, below, inner] = jnp.zeros_like(row_shift)

        widen(r, c, top, bottom)
        return carry

    lax.fori_loop(0, rows * steps, own_rows, 0)

    def relaxed(source, r, c):
        inner = pl.ds(pl.multiple_of(c + PAD, PAD), WIDTH)
        middle, left, right = lanes_beside(
            source[r, body_layers, pl.ds(c, WIDTH + 2 * PAD)], WIDTH
        )
        upper = pltpu.roll(source[r, pl.ds(0, layers + TILE), inner], 1, 0)[TILE:]
        lower = pltpu.roll(source[r, pl.ds(TILE, layers + TILE), inner], layers + TILE - 1, 0)[
            :layers
        ]
        across = source[r - 1, body_layers, inner] + source[r + 1, body_layers, inner]
        neighbours = across + (left + right) + (upper + lower)
        return (1.0 - RELAX_WEIGHT) * middle + (RELAX_WEIGHT / 6.0) * neighbours

    def sweep_once(r, c):
        inner = pl.ds(pl.multiple_of(c + PAD, PAD), WIDTH)
        second[r, body_layers, inner] = relaxed(first, r, c)

    def sweep_twice(r, c):
        value = relaxed(second, r, c)
        result[r - 1, :, pl.ds(c, WIDTH)] = value
        power = value * value
        part = jnp.zeros((TILE, PAD), jnp.float32)
        for top in range(0, layers, TILE):
            for start in range(0, WIDTH, PAD):
                part = part + power[top : top + TILE, start : start + PAD]
        squares[r - 1] = squares[r - 1] + part

    def over(low, count, visit):
        def body(t, carry):
            c = pl.multiple_of(lax.rem(t, steps) * WIDTH, WIDTH)
            visit(t // steps + low, c)
            return carry

        lax.fori_loop(0, count * steps, body, 0)

    over(2, rows - 2, sweep_once)
    for side in (0, 1):
        pl.when(depth_sends[side])(later_layers[0][side].start)

    per_piece = piece // WIDTH
    for side in (0, 1):
        pl.when(lat_recvs[side])(shift_copies[side].wait_recv)
    for k in range(CHUNKS):
        for side in (0, 1):

            @pl.when(lat_recvs[side])
            def _(side=side, k=k):
                first_copies[k][side].wait_recv()
                for j in range(per_piece):
                    widen(far_edge[side], k * piece + j * WIDTH, None, None)

            near = own_edge[1 - side]
            for j in range(per_piece):
                sweep_once(near, k * piece + j * WIDTH)
            pl.when(lat_sends[1 - side])(second_copies[k][1 - side].start)
    for j in (1, 2):
        for side in (0, 1):
            pl.when(depth_sends[side])(later_layers[j][side].start)

    for side in (0, 1):
        pl.when(depth_recvs[side])(later_layers[0][side].wait_recv)
    over(3, rows - 4, sweep_twice)
    over(2, 1, sweep_twice)
    over(rows - 1, 1, sweep_twice)
    inside = pltpu.make_async_copy(
        result.at[pl.ds(1, rows - 2)], field.at[pl.ds(1, rows - 2)], out_sem.at[1]
    )
    inside.start()
    for j in (1, 2):
        for side in (0, 1):
            pl.when(depth_recvs[side])(later_layers[j][side].wait_recv)
    outs = []
    for k in range(CHUNKS):
        for side in (0, 1):
            pl.when(lat_recvs[side])(second_copies[k][side].wait_recv)
            near = own_edge[1 - side]
            for j in range(per_piece):
                sweep_twice(near, k * piece + j * WIDTH)
            cols = pl.ds(k * piece, piece)
            out = pltpu.make_async_copy(
                result.at[near - 1, :, cols],
                field.at[near - 1, :, cols],
                out_sem.at[2 + 2 * k + side],
            )
            out.start()
            outs.append(out)

    sums[...] = jnp.sum(squares[...], axis=1)
    for copy in sum_copies:
        copy.start()
    surface_out.wait()
    inside.wait()
    for side in (0, 1):
        for copy in [surf_copies[side], shift_copies[side]] + [
            group[k][side] for group in (first_copies, second_copies) for k in range(CHUNKS)
        ]:
            pl.when(lat_sends[side])(copy.wait_send)
        for copy in [layer_copies[side]] + [later_layers[j][side] for j in range(3)]:
            pl.when(depth_sends[side])(copy.wait_send)
    total = sums[...]
    for k, copy in enumerate(sum_copies):
        copy.wait_recv()
        total = total + others[k]
    column = jnp.sum(total, axis=1, keepdims=True)
    square = jnp.broadcast_to(column, (rows, norm.shape[1]))
    ids = lax.broadcasted_iota(jnp.int32, square.shape, 0)
    lanes = lax.broadcasted_iota(jnp.int32, square.shape, 1)
    flat = jnp.sum(jnp.where(ids == lanes, square, 0.0), axis=0, keepdims=True)
    norm[...] = jnp.broadcast_to(jnp.sqrt(flat / (total_layers * columns)), norm.shape)
    for copy in sum_copies:
        copy.wait_send()
    for out in outs:
        out.wait()


def solution(mesh):
    lats, depths = mesh.shape["lat"], mesh.shape["depth"]

    def per_device(surface, velocity, block_map, free_flags, block_rates, previous_mesh):
        rows, layers, columns = previous_mesh.shape
        wide = columns + 2 * PAD
        anywhere = pl.BlockSpec(memory_space=pltpu.HBM)
        f32 = jnp.float32
        slots = 2 + 2 * CHUNKS
        others = max(depths - 1, 1)
        new_surface, field, norm = pl.pallas_call(
            functools.partial(kernel, lats, depths),
            out_shape=(
                jax.ShapeDtypeStruct(surface.shape, f32),
                jax.ShapeDtypeStruct(previous_mesh.shape, f32),
                jax.ShapeDtypeStruct((TILE, pl.cdiv(rows, PAD) * PAD), f32),
            ),
            in_specs=[anywhere] * 4 + [pl.BlockSpec(memory_space=pltpu.SMEM), anywhere],
            out_specs=(anywhere, anywhere, pl.BlockSpec(memory_space=pltpu.VMEM)),
            scratch_shapes=[
                pltpu.VMEM((rows + 2 * TILE, wide), f32),
                pltpu.VMEM(velocity.shape, f32),
                pltpu.VMEM(block_map.shape, jnp.int32),
                pltpu.VMEM(free_flags.shape, jnp.int32),
                pltpu.VMEM((rows + 2 * TILE, columns), f32),
                pltpu.VMEM(surface.shape, f32),
                pltpu.VMEM((rows + 2, layers + 2 * TILE, wide), f32),
                pltpu.VMEM((rows + 2, layers + 2 * TILE, wide), f32),
                pltpu.VMEM(previous_mesh.shape, f32),
                pltpu.VMEM((rows, TILE, PAD), f32),
                pltpu.VMEM((rows, PAD), f32),
                pltpu.VMEM((others, rows, PAD), f32),
                pltpu.SemaphoreType.DMA((5,)),
                pltpu.SemaphoreType.DMA((2 + 2 * CHUNKS,)),
                pltpu.SemaphoreType.DMA((2, slots)),
                pltpu.SemaphoreType.DMA((2, slots)),
                pltpu.SemaphoreType.DMA((2, 4)),
                pltpu.SemaphoreType.DMA((2, 4)),
                pltpu.SemaphoreType.DMA((others,)),
                pltpu.SemaphoreType.DMA((others,)),
            ],
            compiler_params=pltpu.CompilerParams(
                collective_id=0, has_side_effects=True, vmem_limit_bytes=62 * 1024 * 1024
            ),
            name="advect_and_relax",
        )(surface, velocity, block_map, free_flags, block_rates, previous_mesh)
        return new_surface, field, norm[0, :rows]

    return jax.shard_map(
        per_device,
        mesh=mesh,
        in_specs=(
            P("lat", None),
            P(None, "lat", None),
            P("lat", None),
            P("lat", None),
            P(),
            P("lat", "depth", None),
        ),
        out_specs=(P("lat", None), P("lat", "depth", None), P("lat")),
        check_vma=False,
    )
```

```python
import functools

import jax
import jax.numpy as jnp
from jax import lax
from jax.experimental import pallas as pl
from jax.experimental.pallas import tpu as pltpu
from jax.sharding import PartitionSpec as P

ITERS = 2
TIME_STEP = 0.5
RELAX_WEIGHT = 0.8
MESH = pl.DeviceIdType.MESH
PAD = 128
TILE = 8
WIDTH = 512
CHUNKS = 4
EARLY = 3
SURF, SHIFT, FIRST = 0, 1, 2


def lanes_beside(window, width):
    span = window.shape[1]
    left = pltpu.roll(window, 1, 1)[:, PAD : PAD + width]
    right = pltpu.roll(window, span - 1, 1)[:, PAD : PAD + width]
    return window[:, PAD : PAD + width], left, right


def kernel(
    lats,
    depths,
    surface,
    velocity,
    block_map,
    free_flags,
    rates,
    previous,
    new_surface,
    field,
    norm,
    surf,
    vel,
    blocks,
    flags,
    shift,
    moved,
    first,
    second,
    result,
    squares,
    sums,
    others,
    local_sem,
    out_sem,
    lat_send,
    lat_recv,
    depth_send,
    depth_recv,
    sum_send,
    sum_recv,
):
    rows, layers, columns = previous.shape
    lat = lax.axis_index("lat")
    depth = lax.axis_index("depth")
    total_layers = layers * depths
    blocks_count = rates.shape[0]
    steps = columns // WIDTH
    piece = columns // CHUNKS
    has_low, has_high = lat > 0, lat < lats - 1
    has_above, has_below = depth > 0, depth < depths - 1
    body_rows = pl.ds(TILE, rows)
    body_layers = pl.ds(TILE, layers)
    body_cols = pl.ds(PAD, columns)

    locals_ = [
        pltpu.make_async_copy(surface, surf.at[body_rows, body_cols], local_sem.at[0]),
        pltpu.make_async_copy(velocity, vel, local_sem.at[1]),
        pltpu.make_async_copy(block_map, blocks, local_sem.at[2]),
        pltpu.make_async_copy(free_flags, flags, local_sem.at[3]),
        pltpu.make_async_copy(
            previous, first.at[pl.ds(1, rows), body_layers, body_cols], local_sem.at[4]
        ),
    ]
    for copy in locals_:
        copy.start()

    barrier = pltpu.get_barrier_semaphore()

    def greet(target):
        pl.semaphore_signal(barrier, inc=1, device_id=target, device_id_type=MESH)

    low_id = {"lat": jnp.maximum(lat - 1, 0)}
    high_id = {"lat": jnp.minimum(lat + 1, lats - 1)}
    above_id = {"depth": jnp.maximum(depth - 1, 0)}
    below_id = {"depth": jnp.minimum(depth + 1, depths - 1)}

    pl.when(has_low)(lambda: greet(low_id))
    pl.when(has_high)(lambda: greet(high_id))
    for k in range(1, depths):
        greet({"depth": lax.rem(depth + k, depths)})
    peers = depths - 1 + has_low.astype(jnp.int32) + has_high.astype(jnp.int32)
    pl.semaphore_wait(barrier, peers)

    def lateral(side, slot, src, dst):
        return pltpu.make_async_remote_copy(
            src_ref=src,
            dst_ref=dst,
            send_sem=lat_send.at[side, slot],
            recv_sem=lat_recv.at[side, slot],
            device_id=high_id if side == 0 else low_id,
            device_id_type=MESH,
        )

    def vertical(side, slot, src, dst):
        return pltpu.make_async_remote_copy(
            src_ref=src,
            dst_ref=dst,
            send_sem=depth_send.at[side, slot],
            recv_sem=depth_recv.at[side, slot],
            device_id=below_id if side == 0 else above_id,
            device_id_type=MESH,
        )

    def piece_cols(k):
        return pl.ds(PAD + k * piece, piece)

    lat_sends = (has_high, has_low)
    lat_recvs = (has_low, has_high)
    depth_sends = (has_below, has_above)
    depth_recvs = (has_above, has_below)
    own_edge = (rows, 1)
    far_edge = (0, rows + 1)
    own_layer = (TILE + layers - 1, TILE)
    far_layer = (TILE - 1, TILE + layers)

    surf_copies = [
        lateral(
            side,
            SURF,
            surface.at[pl.ds((rows - 1, 0)[side], 1), :],
            surf.at[pl.ds((TILE - 1, TILE + rows)[side], 1), body_cols],
        )
        for side in (0, 1)
    ]
    shift_copies = [
        lateral(
            side,
            SHIFT,
            shift.at[pl.ds((TILE + rows - 1, TILE)[side], 1), :],
            shift.at[pl.ds((TILE - 1, TILE + rows)[side], 1), :],
        )
        for side in (0, 1)
    ]
    first_copies = [
        [
            lateral(
                side,
                FIRST + k,
                previous.at[(rows - 1, 0)[side], :, pl.ds(k * piece, piece)],
                first.at[far_edge[side], body_layers, piece_cols(k)],
            )
            for side in (0, 1)
        ]
        for k in range(CHUNKS)
    ]
    second_copies = [
        [
            lateral(
                side,
                FIRST + CHUNKS + k,
                second.at[own_edge[side], body_layers, piece_cols(k)],
                second.at[far_edge[side], body_layers, piece_cols(k)],
            )
            for side in (0, 1)
        ]
        for k in range(CHUNKS)
    ]
    layer_copies = [
        vertical(
            side,
            0,
            previous.at[:, pl.ds((layers - 1, 0)[side], 1), :],
            first.at[pl.ds(1, rows), pl.ds(far_layer[side], 1), body_cols],
        )
        for side in (0, 1)
    ]
    spans = (pl.ds(2, rows - 2), pl.ds(1, 1), pl.ds(rows, 1))
    later_layers = [
        [
            vertical(
                side,
                1 + j,
                second.at[span, pl.ds(own_layer[side], 1), body_cols],
                second.at[span, pl.ds(far_layer[side], 1), body_cols],
            )
            for side in (0, 1)
        ]
        for j, span in enumerate(spans)
    ]
    sum_copies = [
        pltpu.make_async_remote_copy(
            src_ref=sums,
            dst_ref=others.at[k - 1],
            send_sem=sum_send.at[k - 1],
            recv_sem=sum_recv.at[k - 1],
            device_id={"depth": lax.rem(depth + k, depths)},
            device_id_type=MESH,
        )
        for k in range(1, depths)
    ]

    for side in (0, 1):
        pl.when(lat_sends[side])(surf_copies[side].start)
    for side in (0, 1):
        pl.when(depth_sends[side])(layer_copies[side].start)
    for k in range(EARLY):
        for side in (0, 1):
            pl.when(lat_sends[side])(first_copies[k][side].start)

    zero_tile = jnp.zeros((layers, PAD), jnp.float32)

    def clear_pads(r, carry):
        for buffer in (first, second):
            for start in (0, PAD + columns):
                buffer[r, body_layers, pl.ds(start, PAD)] = zero_tile
        return carry

    lax.fori_loop(1, rows + 1, clear_pads, 0)
    for start in (0, PAD + columns):
        surf[body_rows, pl.ds(start, PAD)] = jnp.zeros((rows, PAD), jnp.float32)
    squares[...] = jnp.zeros_like(squares)

    for side in (0, 1):

        @pl.when(jnp.logical_not(lat_recvs[side]))
        def _(side=side):
            surf[pl.ds((TILE - 1, TILE + rows)[side], 1), body_cols] = jnp.zeros(
                (1, columns), jnp.float32
            )
            shift[pl.ds((TILE - 1, TILE + rows)[side], 1), :] = jnp.zeros(
                (1, columns), jnp.float32
            )
            for buffer in (first, second):
                buffer[far_edge[side], body_layers, body_cols] = jnp.zeros(
                    (layers, columns), jnp.float32
                )

    for copy in locals_[:4]:
        copy.wait()
    for side in (0, 1):
        pl.when(lat_recvs[side])(surf_copies[side].wait_recv)

    def advect(step, carry):
        c = pl.multiple_of(step * WIDTH, WIDTH)
        cols = pl.ds(c, WIDTH)
        inner = pl.ds(pl.multiple_of(c + PAD, PAD), WIDTH)
        middle, left, right = lanes_beside(surf[body_rows, pl.ds(c, WIDTH + 2 * PAD)], WIDTH)
        before = pltpu.roll(surf[pl.ds(0, rows + TILE), inner], 1, 0)[TILE:]
        after = pltpu.roll(surf[pl.ds(TILE, rows + TILE), inner], rows + TILE - 1, 0)[:rows]
        grad_rows = (after - before) * 0.5
        grad_cols = (right - left) * 0.5
        laplace = after + before + right + left - 4.0 * middle
        names = blocks[:, cols]
        rate = jnp.full(names.shape, rates[0], jnp.float32)
        for label in range(1, blocks_count):
            rate = jnp.where(names == label, rates[label], rate)
        tendency = -vel[0, :, cols] * grad_rows - vel[1, :, cols] * grad_cols + rate * laplace
        fresh = middle + TIME_STEP * flags[:, cols].astype(jnp.float32) * tendency
        moved[:, cols] = fresh
        shift[body_rows, cols] = fresh - middle
        return carry

    lax.fori_loop(0, steps, advect, 0)
    surface_out = pltpu.make_async_copy(moved, new_surface, out_sem.at[0])
    surface_out.start()
    locals_[4].wait()
    for side in (0, 1):
        pl.when(lat_sends[side])(shift_copies[side].start)
    for k in range(EARLY, CHUNKS):
        for side in (0, 1):
            pl.when(lat_sends[side])(first_copies[k][side].start)

    for side in (0, 1):
        pl.when(depth_recvs[side])(layer_copies[side].wait_recv)

    def profile_of(index):
        return (total_layers - index).astype(jnp.float32) / total_layers

    base = depth * layers
    profile = profile_of(base + lax.broadcasted_iota(jnp.int32, (layers, PAD), 0))
    above_profile = profile_of(base - 1)
    below_profile = profile_of(base + layers)
    sublane = lax.broadcasted_iota(jnp.int32, (layers, WIDTH), 0)
    at_first = sublane == 0
    at_last = sublane == layers - 1
    above = pl.ds(TILE - 1, 1)
    below = pl.ds(TILE + layers, 1)

    def widen(r, c):
        inner = pl.ds(c + PAD, WIDTH)
        row_shift = jnp.broadcast_to(shift[pl.ds(TILE - 1 + r, 1), pl.ds(c, WIDTH)], (layers, WIDTH))
        wide_profile = jnp.concatenate([profile] * (WIDTH // PAD), axis=1)
        first[r, body_layers, inner] = first[r, body_layers, inner] + row_shift * wide_profile

    def relaxed(source, r, c, top, bottom):
        inner = pl.ds(c + PAD, WIDTH)
        middle, left, right = lanes_beside(
            source[r, body_layers, pl.ds(c, WIDTH + 2 * PAD)], WIDTH
        )
        upper = jnp.where(at_first, top, pltpu.roll(middle, 1, 0))
        lower = jnp.where(at_last, bottom, pltpu.roll(middle, layers - 1, 0))
        across = source[r - 1, body_layers, inner] + source[r + 1, body_layers, inner]
        neighbours = across + (left + right) + (upper + lower)
        return (1.0 - RELAX_WEIGHT) * middle + (RELAX_WEIGHT / 6.0) * neighbours

    def sweep_once(r, c):
        inner = pl.ds(c + PAD, WIDTH)
        row_shift = shift[pl.ds(TILE - 1 + r, 1), pl.ds(c, WIDTH)]
        top = jnp.where(has_above, first[r, above, inner] + row_shift * above_profile, row_shift)
        bottom = jnp.where(has_below, first[r, below, inner] + row_shift * below_profile, 0.0)
        second[r, body_layers, inner] = relaxed(first, r, c, top, bottom)

    def sweep_twice(r, c):
        inner = pl.ds(c + PAD, WIDTH)
        row_shift = shift[pl.ds(TILE - 1 + r, 1), pl.ds(c, WIDTH)]
        top = jnp.where(has_above, second[r, above, inner], row_shift)
        bottom = jnp.where(has_below, second[r, below, inner], 0.0)
        value = relaxed(second, r, c, top, bottom)
        result[r - 1, :, pl.ds(c, WIDTH)] = value
        power = value * value
        part = squares[r - 1]
        for top in range(0, layers, TILE):
            for start in range(0, WIDTH, PAD):
                part = part + power[top : top + TILE, start : start + PAD]
        squares[r - 1] = part

    def over(low, count, visit):
        def body(t, carry):
            for step in range(steps):
                visit(t, step * WIDTH)
            return carry

        lax.fori_loop(low, low + count, body, 0)

    over(1, rows, widen)
    over(2, rows - 2, sweep_once)
    for side in (0, 1):
        pl.when(depth_sends[side])(later_layers[0][side].start)

    per_piece = piece // WIDTH
    for side in (0, 1):
        pl.when(lat_recvs[side])(shift_copies[side].wait_recv)
    for k in range(CHUNKS):
        for side in (0, 1):

            @pl.when(lat_recvs[side])
            def _(side=side, k=k):
                first_copies[k][side].wait_recv()
                for j in range(per_piece):
                    widen(far_edge[side], k * piece + j * WIDTH)

            near = own_edge[1 - side]
            for j in range(per_piece):
                sweep_once(near, k * piece + j * WIDTH)
            pl.when(lat_sends[1 - side])(second_copies[k][1 - side].start)
    for j in (1, 2):
        for side in (0, 1):
            pl.when(depth_sends[side])(later_layers[j][side].start)

    for side in (0, 1):
        pl.when(depth_recvs[side])(later_layers[0][side].wait_recv)
    over(3, rows - 4, sweep_twice)
    over(2, 1, sweep_twice)
    over(rows - 1, 1, sweep_twice)
    inside = pltpu.make_async_copy(
        result.at[pl.ds(1, rows - 2)], field.at[pl.ds(1, rows - 2)], out_sem.at[1]
    )
    inside.start()
    for j in (1, 2):
        for side in (0, 1):
            pl.when(depth_recvs[side])(later_layers[j][side].wait_recv)
    outs = []
    for k in range(CHUNKS):
        for side in (0, 1):
            pl.when(lat_recvs[side])(second_copies[k][side].wait_recv)
            near = own_edge[1 - side]
            for j in range(per_piece):
                sweep_twice(near, k * piece + j * WIDTH)
            cols = pl.ds(k * piece, piece)
            out = pltpu.make_async_copy(
                result.at[near - 1, :, cols],
                field.at[near - 1, :, cols],
                out_sem.at[2 + 2 * k + side],
            )
            out.start()
            outs.append(out)

    sums[...] = jnp.sum(squares[...], axis=1)
    for copy in sum_copies:
        copy.start()
    surface_out.wait()
    inside.wait()
    for side in (0, 1):
        for copy in [surf_copies[side], shift_copies[side]] + [
            group[k][side] for group in (first_copies, second_copies) for k in range(CHUNKS)
        ]:
            pl.when(lat_sends[side])(copy.wait_send)
        for copy in [layer_copies[side]] + [later_layers[j][side] for j in range(3)]:
            pl.when(depth_sends[side])(copy.wait_send)
    total = sums[...]
    for k, copy in enumerate(sum_copies):
        copy.wait_recv()
        total = total + others[k]
    column = jnp.sum(total, axis=1, keepdims=True)
    square = jnp.broadcast_to(column, (rows, norm.shape[1]))
    ids = lax.broadcasted_iota(jnp.int32, square.shape, 0)
    lanes = lax.broadcasted_iota(jnp.int32, square.shape, 1)
    flat = jnp.sum(jnp.where(ids == lanes, square, 0.0), axis=0, keepdims=True)
    norm[...] = jnp.broadcast_to(jnp.sqrt(flat / (total_layers * columns)), norm.shape)
    for copy in sum_copies:
        copy.wait_send()
    for out in outs:
        out.wait()


def solution(mesh):
    lats, depths = mesh.shape["lat"], mesh.shape["depth"]

    def per_device(surface, velocity, block_map, free_flags, block_rates, previous_mesh):
        rows, layers, columns = previous_mesh.shape
        wide = columns + 2 * PAD
        anywhere = pl.BlockSpec(memory_space=pltpu.HBM)
        f32 = jnp.float32
        slots = 2 + 2 * CHUNKS
        others = max(depths - 1, 1)
        new_surface, field, norm = pl.pallas_call(
            functools.partial(kernel, lats, depths),
            out_shape=(
                jax.ShapeDtypeStruct(surface.shape, f32),
                jax.ShapeDtypeStruct(previous_mesh.shape, f32),
                jax.ShapeDtypeStruct((TILE, pl.cdiv(rows, PAD) * PAD), f32),
            ),
            in_specs=[anywhere] * 4 + [pl.BlockSpec(memory_space=pltpu.SMEM), anywhere],
            out_specs=(anywhere, anywhere, pl.BlockSpec(memory_space=pltpu.VMEM)),
            scratch_shapes=[
                pltpu.VMEM((rows + 2 * TILE, wide), f32),
                pltpu.VMEM(velocity.shape, f32),
                pltpu.VMEM(block_map.shape, jnp.int32),
                pltpu.VMEM(free_flags.shape, jnp.int32),
                pltpu.VMEM((rows + 2 * TILE, columns), f32),
                pltpu.VMEM(surface.shape, f32),
                pltpu.VMEM((rows + 2, layers + 2 * TILE, wide), f32),
                pltpu.VMEM((rows + 2, layers + 2 * TILE, wide), f32),
                pltpu.VMEM(previous_mesh.shape, f32),
                pltpu.VMEM((rows, TILE, PAD), f32),
                pltpu.VMEM((rows, PAD), f32),
                pltpu.VMEM((others, rows, PAD), f32),
                pltpu.SemaphoreType.DMA((5,)),
                pltpu.SemaphoreType.DMA((2 + 2 * CHUNKS,)),
                pltpu.SemaphoreType.DMA((2, slots)),
                pltpu.SemaphoreType.DMA((2, slots)),
                pltpu.SemaphoreType.DMA((2, 4)),
                pltpu.SemaphoreType.DMA((2, 4)),
                pltpu.SemaphoreType.DMA((others,)),
                pltpu.SemaphoreType.DMA((others,)),
            ],
            compiler_params=pltpu.CompilerParams(
                collective_id=0, has_side_effects=True, vmem_limit_bytes=62 * 1024 * 1024
            ),
            name="advect_and_relax",
        )(surface, velocity, block_map, free_flags, block_rates, previous_mesh)
        return new_surface, field, norm[0, :rows]

    return jax.shard_map(
        per_device,
        mesh=mesh,
        in_specs=(
            P("lat", None),
            P(None, "lat", None),
            P("lat", None),
            P("lat", None),
            P(),
            P("lat", "depth", None),
        ),
        out_specs=(P("lat", None), P("lat", "depth", None), P("lat")),
        check_vma=False,
    )
```

```python
import functools

import jax
import jax.numpy as jnp
from jax import lax
from jax.experimental import pallas as pl
from jax.experimental.pallas import tpu as pltpu
from jax.sharding import PartitionSpec as P

ITERS = 2
TIME_STEP = 0.5
RELAX_WEIGHT = 0.8
MESH = pl.DeviceIdType.MESH
PAD = 128
TILE = 8
WIDTH = 512
CHUNKS = 4
EARLY = 3
SURF, SHIFT, FIRST = 0, 1, 2


def lanes_beside(window, width):
    span = window.shape[1]
    left = pltpu.roll(window, 1, 1)[:, PAD : PAD + width]
    right = pltpu.roll(window, span - 1, 1)[:, PAD : PAD + width]
    return window[:, PAD : PAD + width], left, right


def kernel(
    lats,
    depths,
    surface,
    velocity,
    block_map,
    free_flags,
    rates,
    previous,
    new_surface,
    field,
    norm,
    surf,
    vel,
    blocks,
    flags,
    shift,
    first,
    second,
    squares,
    sums,
    others,
    local_sem,
    lat_send,
    lat_recv,
    depth_send,
    depth_recv,
    sum_send,
    sum_recv,
):
    rows, layers, columns = previous.shape
    lat = lax.axis_index("lat")
    depth = lax.axis_index("depth")
    total_layers = layers * depths
    blocks_count = rates.shape[0]
    steps = columns // WIDTH
    piece = columns // CHUNKS
    has_low, has_high = lat > 0, lat < lats - 1
    has_above, has_below = depth > 0, depth < depths - 1
    body_rows = pl.ds(TILE, rows)
    body_layers = pl.ds(TILE, layers)
    body_cols = pl.ds(PAD, columns)

    locals_ = [
        pltpu.make_async_copy(surface, surf.at[body_rows, body_cols], local_sem.at[0]),
        pltpu.make_async_copy(velocity, vel, local_sem.at[1]),
        pltpu.make_async_copy(block_map, blocks, local_sem.at[2]),
        pltpu.make_async_copy(free_flags, flags, local_sem.at[3]),
        pltpu.make_async_copy(
            previous, first.at[pl.ds(1, rows), body_layers, body_cols], local_sem.at[4]
        ),
    ]
    for copy in locals_:
        copy.start()

    barrier = pltpu.get_barrier_semaphore()

    def greet(target):
        pl.semaphore_signal(barrier, inc=1, device_id=target, device_id_type=MESH)

    low_id = {"lat": jnp.maximum(lat - 1, 0)}
    high_id = {"lat": jnp.minimum(lat + 1, lats - 1)}
    above_id = {"depth": jnp.maximum(depth - 1, 0)}
    below_id = {"depth": jnp.minimum(depth + 1, depths - 1)}

    pl.when(has_low)(lambda: greet(low_id))
    pl.when(has_high)(lambda: greet(high_id))
    for k in range(1, depths):
        greet({"depth": lax.rem(depth + k, depths)})
    peers = depths - 1 + has_low.astype(jnp.int32) + has_high.astype(jnp.int32)
    pl.semaphore_wait(barrier, peers)

    def lateral(side, slot, src, dst):
        return pltpu.make_async_remote_copy(
            src_ref=src,
            dst_ref=dst,
            send_sem=lat_send.at[side, slot],
            recv_sem=lat_recv.at[side, slot],
            device_id=high_id if side == 0 else low_id,
            device_id_type=MESH,
        )

    def vertical(side, slot, src, dst):
        return pltpu.make_async_remote_copy(
            src_ref=src,
            dst_ref=dst,
            send_sem=depth_send.at[side, slot],
            recv_sem=depth_recv.at[side, slot],
            device_id=below_id if side == 0 else above_id,
            device_id_type=MESH,
        )

    def piece_cols(k):
        return pl.ds(PAD + k * piece, piece)

    lat_sends = (has_high, has_low)
    lat_recvs = (has_low, has_high)
    depth_sends = (has_below, has_above)
    depth_recvs = (has_above, has_below)
    own_edge = (rows, 1)
    far_edge = (0, rows + 1)
    own_layer = (TILE + layers - 1, TILE)
    far_layer = (TILE - 1, TILE + layers)

    surf_copies = [
        lateral(
            side,
            SURF,
            surface.at[pl.ds((rows - 1, 0)[side], 1), :],
            surf.at[pl.ds((TILE - 1, TILE + rows)[side], 1), body_cols],
        )
        for side in (0, 1)
    ]
    shift_copies = [
        lateral(
            side,
            SHIFT,
            shift.at[pl.ds((TILE + rows - 1, TILE)[side], 1), :],
            shift.at[pl.ds((TILE - 1, TILE + rows)[side], 1), :],
        )
        for side in (0, 1)
    ]
    first_copies = [
        [
            lateral(
                side,
                FIRST + k,
                previous.at[(rows - 1, 0)[side], :, pl.ds(k * piece, piece)],
                first.at[far_edge[side], body_layers, piece_cols(k)],
            )
            for side in (0, 1)
        ]
        for k in range(CHUNKS)
    ]
    second_copies = [
        [
            lateral(
                side,
                FIRST + CHUNKS + k,
                second.at[own_edge[side], body_layers, piece_cols(k)],
                second.at[far_edge[side], body_layers, piece_cols(k)],
            )
            for side in (0, 1)
        ]
        for k in range(CHUNKS)
    ]
    layer_copies = [
        vertical(
            side,
            0,
            previous.at[:, pl.ds((layers - 1, 0)[side], 1), :],
            first.at[pl.ds(1, rows), pl.ds(far_layer[side], 1), body_cols],
        )
        for side in (0, 1)
    ]
    spans = (pl.ds(2, rows - 2), pl.ds(1, 1), pl.ds(rows, 1))
    later_layers = [
        [
            vertical(
                side,
                1 + j,
                second.at[span, pl.ds(own_layer[side], 1), body_cols],
                second.at[span, pl.ds(far_layer[side], 1), body_cols],
            )
            for side in (0, 1)
        ]
        for j, span in enumerate(spans)
    ]
    sum_copies = [
        pltpu.make_async_remote_copy(
            src_ref=sums,
            dst_ref=others.at[k - 1],
            send_sem=sum_send.at[k - 1],
            recv_sem=sum_recv.at[k - 1],
            device_id={"depth": lax.rem(depth + k, depths)},
            device_id_type=MESH,
        )
        for k in range(1, depths)
    ]

    for side in (0, 1):
        pl.when(lat_sends[side])(surf_copies[side].start)
    for side in (0, 1):
        pl.when(depth_sends[side])(layer_copies[side].start)
    for k in range(EARLY):
        for side in (0, 1):
            pl.when(lat_sends[side])(first_copies[k][side].start)

    zero_tile = jnp.zeros((layers, PAD), jnp.float32)

    def clear_pads(r, carry):
        for buffer in (first, second):
            for start in (0, PAD + columns):
                buffer[r, body_layers, pl.ds(start, PAD)] = zero_tile
        return carry

    lax.fori_loop(1, rows + 1, clear_pads, 0)
    for start in (0, PAD + columns):
        surf[body_rows, pl.ds(start, PAD)] = jnp.zeros((rows, PAD), jnp.float32)
    squares[...] = jnp.zeros_like(squares)

    for side in (0, 1):

        @pl.when(jnp.logical_not(lat_recvs[side]))
        def _(side=side):
            surf[pl.ds((TILE - 1, TILE + rows)[side], 1), body_cols] = jnp.zeros(
                (1, columns), jnp.float32
            )
            shift[pl.ds((TILE - 1, TILE + rows)[side], 1), :] = jnp.zeros(
                (1, columns), jnp.float32
            )
            for buffer in (first, second):
                buffer[far_edge[side], body_layers, body_cols] = jnp.zeros(
                    (layers, columns), jnp.float32
                )

    for copy in locals_[:4]:
        copy.wait()
    for side in (0, 1):
        pl.when(lat_recvs[side])(surf_copies[side].wait_recv)

    def advect(step, carry):
        c = pl.multiple_of(step * WIDTH, WIDTH)
        cols = pl.ds(c, WIDTH)
        inner = pl.ds(pl.multiple_of(c + PAD, PAD), WIDTH)
        middle, left, right = lanes_beside(surf[body_rows, pl.ds(c, WIDTH + 2 * PAD)], WIDTH)
        before = pltpu.roll(surf[pl.ds(0, rows + TILE), inner], 1, 0)[TILE:]
        after = pltpu.roll(surf[pl.ds(TILE, rows + TILE), inner], rows + TILE - 1, 0)[:rows]
        grad_rows = (after - before) * 0.5
        grad_cols = (right - left) * 0.5
        laplace = after + before + right + left - 4.0 * middle
        names = blocks[:, cols]
        rate = jnp.full(names.shape, rates[0], jnp.float32)
        for label in range(1, blocks_count):
            rate = jnp.where(names == label, rates[label], rate)
        tendency = -vel[0, :, cols] * grad_rows - vel[1, :, cols] * grad_cols + rate * laplace
        fresh = middle + TIME_STEP * flags[:, cols].astype(jnp.float32) * tendency
        new_surface[:, cols] = fresh
        shift[body_rows, cols] = fresh - middle
        return carry

    lax.fori_loop(0, steps, advect, 0)
    locals_[4].wait()
    for side in (0, 1):
        pl.when(lat_sends[side])(shift_copies[side].start)
    for k in range(EARLY, CHUNKS):
        for side in (0, 1):
            pl.when(lat_sends[side])(first_copies[k][side].start)

    for side in (0, 1):
        pl.when(depth_recvs[side])(layer_copies[side].wait_recv)

    def profile_of(index):
        return (total_layers - index).astype(jnp.float32) / total_layers

    base = depth * layers
    profile = profile_of(base + lax.broadcasted_iota(jnp.int32, (layers, PAD), 0))
    above_profile = profile_of(base - 1)
    below_profile = profile_of(base + layers)
    sublane = lax.broadcasted_iota(jnp.int32, (layers, WIDTH), 0)
    at_first = sublane == 0
    at_last = sublane == layers - 1
    above = pl.ds(TILE - 1, 1)
    below = pl.ds(TILE + layers, 1)

    def widen(r, c):
        inner = pl.ds(c + PAD, WIDTH)
        row_shift = jnp.broadcast_to(shift[pl.ds(TILE - 1 + r, 1), pl.ds(c, WIDTH)], (layers, WIDTH))
        wide_profile = jnp.concatenate([profile] * (WIDTH // PAD), axis=1)
        first[r, body_layers, inner] = first[r, body_layers, inner] + row_shift * wide_profile

    def relaxed(source, r, c, top, bottom):
        inner = pl.ds(c + PAD, WIDTH)
        middle, left, right = lanes_beside(
            source[r, body_layers, pl.ds(c, WIDTH + 2 * PAD)], WIDTH
        )
        upper = jnp.where(at_first, top, pltpu.roll(middle, 1, 0))
        lower = jnp.where(at_last, bottom, pltpu.roll(middle, layers - 1, 0))
        across = source[r - 1, body_layers, inner] + source[r + 1, body_layers, inner]
        neighbours = across + (left + right) + (upper + lower)
        return (1.0 - RELAX_WEIGHT) * middle + (RELAX_WEIGHT / 6.0) * neighbours

    def sweep_once(r, c):
        inner = pl.ds(c + PAD, WIDTH)
        row_shift = shift[pl.ds(TILE - 1 + r, 1), pl.ds(c, WIDTH)]
        top = jnp.where(has_above, first[r, above, inner] + row_shift * above_profile, row_shift)
        bottom = jnp.where(has_below, first[r, below, inner] + row_shift * below_profile, 0.0)
        second[r, body_layers, inner] = relaxed(first, r, c, top, bottom)

    def sweep_twice(r, c):
        inner = pl.ds(c + PAD, WIDTH)
        row_shift = shift[pl.ds(TILE - 1 + r, 1), pl.ds(c, WIDTH)]
        top = jnp.where(has_above, second[r, above, inner], row_shift)
        bottom = jnp.where(has_below, second[r, below, inner], 0.0)
        value = relaxed(second, r, c, top, bottom)
        field[r - 1, :, pl.ds(c, WIDTH)] = value
        power = value * value
        part = squares[r - 1]
        for top in range(0, layers, TILE):
            for start in range(0, WIDTH, PAD):
                part = part + power[top : top + TILE, start : start + PAD]
        squares[r - 1] = part

    def over(low, count, visit):
        def body(t, carry):
            for step in range(steps):
                visit(t, step * WIDTH)
            return carry

        lax.fori_loop(low, low + count, body, 0)

    over(1, rows, widen)
    over(2, rows - 2, sweep_once)
    for side in (0, 1):
        pl.when(depth_sends[side])(later_layers[0][side].start)

    per_piece = piece // WIDTH
    for side in (0, 1):
        pl.when(lat_recvs[side])(shift_copies[side].wait_recv)
    for k in range(CHUNKS):
        for side in (0, 1):

            @pl.when(lat_recvs[side])
            def _(side=side, k=k):
                first_copies[k][side].wait_recv()
                for j in range(per_piece):
                    widen(far_edge[side], k * piece + j * WIDTH)

            near = own_edge[1 - side]
            for j in range(per_piece):
                sweep_once(near, k * piece + j * WIDTH)
            pl.when(lat_sends[1 - side])(second_copies[k][1 - side].start)
    for j in (1, 2):
        for side in (0, 1):
            pl.when(depth_sends[side])(later_layers[j][side].start)

    for side in (0, 1):
        pl.when(depth_recvs[side])(later_layers[0][side].wait_recv)
    over(3, rows - 4, sweep_twice)
    over(2, 1, sweep_twice)
    over(rows - 1, 1, sweep_twice)
    for j in (1, 2):
        for side in (0, 1):
            pl.when(depth_recvs[side])(later_layers[j][side].wait_recv)
    for k in range(CHUNKS):
        for side in (0, 1):
            pl.when(lat_recvs[side])(second_copies[k][side].wait_recv)
            near = own_edge[1 - side]
            for j in range(per_piece):
                sweep_twice(near, k * piece + j * WIDTH)

    sums[...] = jnp.sum(squares[...], axis=1)
    for copy in sum_copies:
        copy.start()
    for side in (0, 1):
        for copy in [surf_copies[side], shift_copies[side]] + [
            group[k][side] for group in (first_copies, second_copies) for k in range(CHUNKS)
        ]:
            pl.when(lat_sends[side])(copy.wait_send)
        for copy in [layer_copies[side]] + [later_layers[j][side] for j in range(3)]:
            pl.when(depth_sends[side])(copy.wait_send)
    total = sums[...]
    for k, copy in enumerate(sum_copies):
        copy.wait_recv()
        total = total + others[k]
    column = jnp.sum(total, axis=1, keepdims=True)
    square = jnp.broadcast_to(column, (rows, norm.shape[1]))
    ids = lax.broadcasted_iota(jnp.int32, square.shape, 0)
    lanes = lax.broadcasted_iota(jnp.int32, square.shape, 1)
    flat = jnp.sum(jnp.where(ids == lanes, square, 0.0), axis=0, keepdims=True)
    norm[...] = jnp.broadcast_to(jnp.sqrt(flat / (total_layers * columns)), norm.shape)
    for copy in sum_copies:
        copy.wait_send()


def solution(mesh):
    lats, depths = mesh.shape["lat"], mesh.shape["depth"]

    def per_device(surface, velocity, block_map, free_flags, block_rates, previous_mesh):
        rows, layers, columns = previous_mesh.shape
        wide = columns + 2 * PAD
        anywhere = pl.BlockSpec(memory_space=pltpu.HBM)
        f32 = jnp.float32
        slots = 2 + 2 * CHUNKS
        others = max(depths - 1, 1)
        held = [
            pltpu.with_memory_space_constraint(value, pltpu.HBM)
            for value in (surface, velocity, block_map, free_flags, previous_mesh)
        ]
        new_surface, field, norm = pl.pallas_call(
            functools.partial(kernel, lats, depths),
            out_shape=(
                pltpu.VMEM(surface.shape, f32),
                pltpu.VMEM(previous_mesh.shape, f32),
                pltpu.VMEM((TILE, pl.cdiv(rows, PAD) * PAD), f32),
            ),
            in_specs=[anywhere] * 4 + [pl.BlockSpec(memory_space=pltpu.SMEM), anywhere],
            out_specs=(pl.BlockSpec(memory_space=pltpu.VMEM),) * 3,
            scratch_shapes=[
                pltpu.VMEM((rows + 2 * TILE, wide), f32),
                pltpu.VMEM(velocity.shape, f32),
                pltpu.VMEM(block_map.shape, jnp.int32),
                pltpu.VMEM(free_flags.shape, jnp.int32),
                pltpu.VMEM((rows + 2 * TILE, columns), f32),
                pltpu.VMEM((rows + 2, layers + 2 * TILE, wide), f32),
                pltpu.VMEM((rows + 2, layers + 2 * TILE, wide), f32),
                pltpu.VMEM((rows, TILE, PAD), f32),
                pltpu.VMEM((rows, PAD), f32),
                pltpu.VMEM((others, rows, PAD), f32),
                pltpu.SemaphoreType.DMA((5,)),
                pltpu.SemaphoreType.DMA((2, slots)),
                pltpu.SemaphoreType.DMA((2, slots)),
                pltpu.SemaphoreType.DMA((2, 4)),
                pltpu.SemaphoreType.DMA((2, 4)),
                pltpu.SemaphoreType.DMA((others,)),
                pltpu.SemaphoreType.DMA((others,)),
            ],
            compiler_params=pltpu.CompilerParams(
                collective_id=0, has_side_effects=True, vmem_limit_bytes=56 * 1024 * 1024
            ),
            name="advect_and_relax",
        )(*held[:4], block_rates, held[4])
        return new_surface, field, norm[0, :rows]

    return jax.shard_map(
        per_device,
        mesh=mesh,
        in_specs=(
            P("lat", None),
            P(None, "lat", None),
            P("lat", None),
            P("lat", None),
            P(),
            P("lat", "depth", None),
        ),
        out_specs=(P("lat", None), P("lat", "depth", None), P("lat")),
        check_vma=False,
    )
```

```python
import functools

import jax
import jax.numpy as jnp
from jax import lax
from jax.experimental import pallas as pl
from jax.experimental.pallas import tpu as pltpu
from jax.sharding import PartitionSpec as P

ITERS = 2
TIME_STEP = 0.5
RELAX_WEIGHT = 0.8
MESH = pl.DeviceIdType.MESH
PAD = 128
TILE = 8
WIDTH = 512
CHUNKS = 4
EARLY = 3
SURF, SHIFT, FIRST = 0, 1, 2


def lanes_beside(window, width):
    span = window.shape[1]
    left = pltpu.roll(window, 1, 1)[:, PAD : PAD + width]
    right = pltpu.roll(window, span - 1, 1)[:, PAD : PAD + width]
    return window[:, PAD : PAD + width], left, right


def kernel(
    lats,
    depths,
    surface,
    velocity,
    block_map,
    free_flags,
    rates,
    previous,
    new_surface,
    field,
    norm,
    surf,
    vel,
    blocks,
    flags,
    shift,
    first,
    second,
    squares,
    sums,
    others,
    local_sem,
    lat_send,
    lat_recv,
    depth_send,
    depth_recv,
    sum_send,
    sum_recv,
):
    rows, layers, columns = previous.shape
    lat = lax.axis_index("lat")
    depth = lax.axis_index("depth")
    total_layers = layers * depths
    blocks_count = rates.shape[0]
    steps = columns // WIDTH
    piece = columns // CHUNKS
    has_low, has_high = lat > 0, lat < lats - 1
    has_above, has_below = depth > 0, depth < depths - 1
    body_rows = pl.ds(TILE, rows)
    body_layers = pl.ds(TILE, layers)
    body_cols = pl.ds(PAD, columns)

    locals_ = [
        pltpu.make_async_copy(surface, surf.at[body_rows, body_cols], local_sem.at[0]),
        pltpu.make_async_copy(velocity, vel, local_sem.at[1]),
        pltpu.make_async_copy(block_map, blocks, local_sem.at[2]),
        pltpu.make_async_copy(free_flags, flags, local_sem.at[3]),
        pltpu.make_async_copy(
            previous, first.at[pl.ds(1, rows), body_layers, body_cols], local_sem.at[4]
        ),
    ]
    for copy in locals_:
        copy.start()

    barrier = pltpu.get_barrier_semaphore()

    def greet(target):
        pl.semaphore_signal(barrier, inc=1, device_id=target, device_id_type=MESH)

    low_id = {"lat": jnp.maximum(lat - 1, 0)}
    high_id = {"lat": jnp.minimum(lat + 1, lats - 1)}
    above_id = {"depth": jnp.maximum(depth - 1, 0)}
    below_id = {"depth": jnp.minimum(depth + 1, depths - 1)}

    pl.when(has_low)(lambda: greet(low_id))
    pl.when(has_high)(lambda: greet(high_id))
    for k in range(1, depths):
        greet({"depth": lax.rem(depth + k, depths)})
    peers = depths - 1 + has_low.astype(jnp.int32) + has_high.astype(jnp.int32)
    pl.semaphore_wait(barrier, peers)

    def lateral(side, slot, src, dst):
        return pltpu.make_async_remote_copy(
            src_ref=src,
            dst_ref=dst,
            send_sem=lat_send.at[side, slot],
            recv_sem=lat_recv.at[side, slot],
            device_id=high_id if side == 0 else low_id,
            device_id_type=MESH,
        )

    def vertical(side, slot, src, dst):
        return pltpu.make_async_remote_copy(
            src_ref=src,
            dst_ref=dst,
            send_sem=depth_send.at[side, slot],
            recv_sem=depth_recv.at[side, slot],
            device_id=below_id if side == 0 else above_id,
            device_id_type=MESH,
        )

    def piece_cols(k):
        return pl.ds(PAD + k * piece, piece)

    lat_sends = (has_high, has_low)
    lat_recvs = (has_low, has_high)
    depth_sends = (has_below, has_above)
    depth_recvs = (has_above, has_below)
    own_edge = (rows, 1)
    far_edge = (0, rows + 1)
    own_layer = (TILE + layers - 1, TILE)
    far_layer = (TILE - 1, TILE + layers)

    surf_copies = [
        lateral(
            side,
            SURF,
            surf.at[pl.ds((TILE + rows - 1, TILE)[side], 1), body_cols],
            surf.at[pl.ds((TILE - 1, TILE + rows)[side], 1), body_cols],
        )
        for side in (0, 1)
    ]
    shift_copies = [
        lateral(
            side,
            SHIFT,
            shift.at[pl.ds((TILE + rows - 1, TILE)[side], 1), :],
            shift.at[pl.ds((TILE - 1, TILE + rows)[side], 1), :],
        )
        for side in (0, 1)
    ]
    first_copies = [
        [
            lateral(
                side,
                FIRST + k,
                previous.at[(rows - 1, 0)[side], :, pl.ds(k * piece, piece)],
                first.at[far_edge[side], body_layers, piece_cols(k)],
            )
            for side in (0, 1)
        ]
        for k in range(CHUNKS)
    ]
    second_copies = [
        [
            lateral(
                side,
                FIRST + CHUNKS + k,
                second.at[own_edge[side], body_layers, piece_cols(k)],
                second.at[far_edge[side], body_layers, piece_cols(k)],
            )
            for side in (0, 1)
        ]
        for k in range(CHUNKS)
    ]
    layer_copies = [
        vertical(
            side,
            0,
            previous.at[:, pl.ds((layers - 1, 0)[side], 1), :],
            first.at[pl.ds(1, rows), pl.ds(far_layer[side], 1), body_cols],
        )
        for side in (0, 1)
    ]
    spans = (pl.ds(2, rows - 2), pl.ds(1, 1), pl.ds(rows, 1))
    later_layers = [
        [
            vertical(
                side,
                1 + j,
                second.at[span, pl.ds(own_layer[side], 1), body_cols],
                second.at[span, pl.ds(far_layer[side], 1), body_cols],
            )
            for side in (0, 1)
        ]
        for j, span in enumerate(spans)
    ]
    sum_copies = [
        pltpu.make_async_remote_copy(
            src_ref=sums,
            dst_ref=others.at[k - 1],
            send_sem=sum_send.at[k - 1],
            recv_sem=sum_recv.at[k - 1],
            device_id={"depth": lax.rem(depth + k, depths)},
            device_id_type=MESH,
        )
        for k in range(1, depths)
    ]

    locals_[0].wait()
    for side in (0, 1):
        pl.when(lat_sends[side])(surf_copies[side].start)
    for side in (0, 1):
        pl.when(depth_sends[side])(layer_copies[side].start)
    for k in range(EARLY):
        for side in (0, 1):
            pl.when(lat_sends[side])(first_copies[k][side].start)

    zero_tile = jnp.zeros((layers, PAD), jnp.float32)

    def clear_pads(r, carry):
        for buffer in (first, second):
            for start in (0, PAD + columns):
                buffer[r, body_layers, pl.ds(start, PAD)] = zero_tile
        return carry

    lax.fori_loop(1, rows + 1, clear_pads, 0)
    for start in (0, PAD + columns):
        surf[body_rows, pl.ds(start, PAD)] = jnp.zeros((rows, PAD), jnp.float32)
    squares[...] = jnp.zeros_like(squares)

    for side in (0, 1):

        @pl.when(jnp.logical_not(lat_recvs[side]))
        def _(side=side):
            surf[pl.ds((TILE - 1, TILE + rows)[side], 1), body_cols] = jnp.zeros(
                (1, columns), jnp.float32
            )
            shift[pl.ds((TILE - 1, TILE + rows)[side], 1), :] = jnp.zeros(
                (1, columns), jnp.float32
            )
            for buffer in (first, second):
                buffer[far_edge[side], body_layers, body_cols] = jnp.zeros(
                    (layers, columns), jnp.float32
                )

    for copy in locals_[1:4]:
        copy.wait()
    for side in (0, 1):
        pl.when(lat_recvs[side])(surf_copies[side].wait_recv)

    def advect(step, carry):
        c = pl.multiple_of(step * WIDTH, WIDTH)
        cols = pl.ds(c, WIDTH)
        inner = pl.ds(pl.multiple_of(c + PAD, PAD), WIDTH)
        middle, left, right = lanes_beside(surf[body_rows, pl.ds(c, WIDTH + 2 * PAD)], WIDTH)
        before = pltpu.roll(surf[pl.ds(0, rows + TILE), inner], 1, 0)[TILE:]
        after = pltpu.roll(surf[pl.ds(TILE, rows + TILE), inner], rows + TILE - 1, 0)[:rows]
        grad_rows = (after - before) * 0.5
        grad_cols = (right - left) * 0.5
        laplace = after + before + right + left - 4.0 * middle
        names = blocks[:, cols]
        rate = jnp.full(names.shape, rates[0], jnp.float32)
        for label in range(1, blocks_count):
            rate = jnp.where(names == label, rates[label], rate)
        tendency = -vel[0, :, cols] * grad_rows - vel[1, :, cols] * grad_cols + rate * laplace
        fresh = middle + TIME_STEP * flags[:, cols].astype(jnp.float32) * tendency
        new_surface[:, cols] = fresh
        shift[body_rows, cols] = fresh - middle
        return carry

    lax.fori_loop(0, steps, advect, 0)
    locals_[4].wait()
    for side in (0, 1):
        pl.when(lat_sends[side])(shift_copies[side].start)
    for k in range(EARLY, CHUNKS):
        for side in (0, 1):
            pl.when(lat_sends[side])(first_copies[k][side].start)

    for side in (0, 1):
        pl.when(depth_recvs[side])(layer_copies[side].wait_recv)

    def profile_of(index):
        return (total_layers - index).astype(jnp.float32) / total_layers

    base = depth * layers
    profile = profile_of(base + lax.broadcasted_iota(jnp.int32, (layers, PAD), 0))
    above_profile = profile_of(base - 1)
    below_profile = profile_of(base + layers)
    sublane = lax.broadcasted_iota(jnp.int32, (layers, WIDTH), 0)
    at_first = sublane == 0
    at_last = sublane == layers - 1
    above = pl.ds(TILE - 1, 1)
    below = pl.ds(TILE + layers, 1)

    def widen(r, c):
        inner = pl.ds(c + PAD, WIDTH)
        row_shift = jnp.broadcast_to(shift[pl.ds(TILE - 1 + r, 1), pl.ds(c, WIDTH)], (layers, WIDTH))
        wide_profile = jnp.concatenate([profile] * (WIDTH // PAD), axis=1)
        first[r, body_layers, inner] = first[r, body_layers, inner] + row_shift * wide_profile

    def relaxed(source, r, c, top, bottom):
        inner = pl.ds(c + PAD, WIDTH)
        middle, left, right = lanes_beside(
            source[r, body_layers, pl.ds(c, WIDTH + 2 * PAD)], WIDTH
        )
        upper = jnp.where(at_first, top, pltpu.roll(middle, 1, 0))
        lower = jnp.where(at_last, bottom, pltpu.roll(middle, layers - 1, 0))
        across = source[r - 1, body_layers, inner] + source[r + 1, body_layers, inner]
        neighbours = across + (left + right) + (upper + lower)
        return (1.0 - RELAX_WEIGHT) * middle + (RELAX_WEIGHT / 6.0) * neighbours

    def sweep_once(r, c):
        inner = pl.ds(c + PAD, WIDTH)
        row_shift = shift[pl.ds(TILE - 1 + r, 1), pl.ds(c, WIDTH)]
        top = jnp.where(has_above, first[r, above, inner] + row_shift * above_profile, row_shift)
        bottom = jnp.where(has_below, first[r, below, inner] + row_shift * below_profile, 0.0)
        second[r, body_layers, inner] = relaxed(first, r, c, top, bottom)

    def sweep_twice(r, c):
        inner = pl.ds(c + PAD, WIDTH)
        row_shift = shift[pl.ds(TILE - 1 + r, 1), pl.ds(c, WIDTH)]
        top = jnp.where(has_above, second[r, above, inner], row_shift)
        bottom = jnp.where(has_below, second[r, below, inner], 0.0)
        value = relaxed(second, r, c, top, bottom)
        field[r - 1, :, pl.ds(c, WIDTH)] = value
        power = value * value
        part = squares[r - 1]
        for top in range(0, layers, TILE):
            for start in range(0, WIDTH, PAD):
                part = part + power[top : top + TILE, start : start + PAD]
        squares[r - 1] = part

    def over(low, count, visit):
        def body(t, carry):
            for step in range(steps):
                visit(t, step * WIDTH)
            return carry

        lax.fori_loop(low, low + count, body, 0)

    over(1, rows, widen)
    over(2, rows - 2, sweep_once)
    for side in (0, 1):
        pl.when(depth_sends[side])(later_layers[0][side].start)

    per_piece = piece // WIDTH
    for side in (0, 1):
        pl.when(lat_recvs[side])(shift_copies[side].wait_recv)
    for k in range(CHUNKS):
        for side in (0, 1):

            @pl.when(lat_recvs[side])
            def _(side=side, k=k):
                first_copies[k][side].wait_recv()
                for j in range(per_piece):
                    widen(far_edge[side], k * piece + j * WIDTH)

            near = own_edge[1 - side]
            for j in range(per_piece):
                sweep_once(near, k * piece + j * WIDTH)
            pl.when(lat_sends[1 - side])(second_copies[k][1 - side].start)
    for j in (1, 2):
        for side in (0, 1):
            pl.when(depth_sends[side])(later_layers[j][side].start)

    for side in (0, 1):
        pl.when(depth_recvs[side])(later_layers[0][side].wait_recv)
    over(3, rows - 4, sweep_twice)
    over(2, 1, sweep_twice)
    over(rows - 1, 1, sweep_twice)
    for j in (1, 2):
        for side in (0, 1):
            pl.when(depth_recvs[side])(later_layers[j][side].wait_recv)
    for k in range(CHUNKS):
        for side in (0, 1):
            pl.when(lat_recvs[side])(second_copies[k][side].wait_recv)
            near = own_edge[1 - side]
            for j in range(per_piece):
                sweep_twice(near, k * piece + j * WIDTH)

    sums[...] = jnp.sum(squares[...], axis=1)
    for copy in sum_copies:
        copy.start()
    for side in (0, 1):
        for copy in [surf_copies[side], shift_copies[side]] + [
            group[k][side] for group in (first_copies, second_copies) for k in range(CHUNKS)
        ]:
            pl.when(lat_sends[side])(copy.wait_send)
        for copy in [layer_copies[side]] + [later_layers[j][side] for j in range(3)]:
            pl.when(depth_sends[side])(copy.wait_send)
    total = sums[...]
    for k, copy in enumerate(sum_copies):
        copy.wait_recv()
        total = total + others[k]
    column = jnp.sum(total, axis=1, keepdims=True)
    square = jnp.broadcast_to(column, (rows, norm.shape[1]))
    ids = lax.broadcasted_iota(jnp.int32, square.shape, 0)
    lanes = lax.broadcasted_iota(jnp.int32, square.shape, 1)
    flat = jnp.sum(jnp.where(ids == lanes, square, 0.0), axis=0, keepdims=True)
    norm[...] = jnp.broadcast_to(jnp.sqrt(flat / (total_layers * columns)), norm.shape)
    for copy in sum_copies:
        copy.wait_send()


def solution(mesh):
    lats, depths = mesh.shape["lat"], mesh.shape["depth"]

    def per_device(surface, velocity, block_map, free_flags, block_rates, previous_mesh):
        rows, layers, columns = previous_mesh.shape
        wide = columns + 2 * PAD
        anywhere = pl.BlockSpec(memory_space=pltpu.HBM)
        f32 = jnp.float32
        slots = 2 + 2 * CHUNKS
        others = max(depths - 1, 1)
        held = [
            pltpu.with_memory_space_constraint(value, pltpu.HBM)
            for value in (surface, velocity, block_map, free_flags, previous_mesh)
        ]
        new_surface, field, norm = pl.pallas_call(
            functools.partial(kernel, lats, depths),
            out_shape=(
                pltpu.VMEM(surface.shape, f32),
                pltpu.VMEM(previous_mesh.shape, f32),
                pltpu.VMEM((TILE, pl.cdiv(rows, PAD) * PAD), f32),
            ),
            in_specs=[anywhere] * 4 + [pl.BlockSpec(memory_space=pltpu.SMEM), anywhere],
            out_specs=(pl.BlockSpec(memory_space=pltpu.VMEM),) * 3,
            scratch_shapes=[
                pltpu.VMEM((rows + 2 * TILE, wide), f32),
                pltpu.VMEM(velocity.shape, f32),
                pltpu.VMEM(block_map.shape, jnp.int32),
                pltpu.VMEM(free_flags.shape, jnp.int32),
                pltpu.VMEM((rows + 2 * TILE, columns), f32),
                pltpu.VMEM((rows + 2, layers + 2 * TILE, wide), f32),
                pltpu.VMEM((rows + 2, layers + 2 * TILE, wide), f32),
                pltpu.VMEM((rows, TILE, PAD), f32),
                pltpu.VMEM((rows, PAD), f32),
                pltpu.VMEM((others, rows, PAD), f32),
                pltpu.SemaphoreType.DMA((5,)),
                pltpu.SemaphoreType.DMA((2, slots)),
                pltpu.SemaphoreType.DMA((2, slots)),
                pltpu.SemaphoreType.DMA((2, 4)),
                pltpu.SemaphoreType.DMA((2, 4)),
                pltpu.SemaphoreType.DMA((others,)),
                pltpu.SemaphoreType.DMA((others,)),
            ],
            compiler_params=pltpu.CompilerParams(
                collective_id=0, has_side_effects=True, vmem_limit_bytes=56 * 1024 * 1024
            ),
            name="advect_and_relax",
        )(*held[:4], block_rates, held[4])
        return new_surface, field, norm[0, :rows]

    return jax.shard_map(
        per_device,
        mesh=mesh,
        in_specs=(
            P("lat", None),
            P(None, "lat", None),
            P("lat", None),
            P("lat", None),
            P(),
            P("lat", "depth", None),
        ),
        out_specs=(P("lat", None), P("lat", "depth", None), P("lat")),
        check_vma=False,
    )
```
